32 devices in a mesh: img: 8 (over z, y), nrn: 4 (over x, core).
Axes of the slice: x: 2, y: 2, z: 4, core: 2. Of those that a mesh axis runs over, the one named last changes fastest.
Arguments:
- images: bfloat16 [2048, 16384], P('img', 'nrn'), may hold values from 0 to 12
- weights: bfloat16 [2, 128, 512, 128], P(None, 'nrn'), may hold values from -0.375 to 0.375
- block_index: int32 [2, 128, 4], replicated, may hold values from 0 to 127, as said below
- bias: float32 [2, 16384], replicated, may hold values from -0.2 to -0.02
Outputs:
- activations: bfloat16 [2048, 16384], P('img', 'nrn')
- live_fraction: float32 [2], replicated
The draws below stay inside these ranges and needn't reach their ends.
Inputs may be any that keep to these rules, and one draw needn't show every extreme that they name: `block_index`: the 4 entries of each row name different blocks.
All inputs are finite; a program needn't handle non-finite values.
Results may differ from the reference program's by a relative error of at most 0.005.
Values may be sent and summed in bfloat16 or wider, within the bound.
No kernel may reach another device: no remote copies, remote signals or barrier semaphores. Data moves between devices by JAX's collectives and lax.ppermute only.
A program may use at most 128 MiB of HBM per device.

```python
import math
import jax
import jax.numpy as jnp
from jax import lax

NEURONS = 16384
TILE = 128
K = 4
LAYERS = 2
IMG_GRP = 256
BLOCKS = 128
N_IMG = 8


def draw_images(key, part):
    first, second, third = jax.random.split(key, 3)
    total_rows = IMG_GRP * N_IMG
    positions = jnp.arange(total_rows, dtype=jnp.float32)
    ramp = 1.0 + 2.0 * positions / max(total_rows - 1, 1)
    scales = jnp.exp(jax.random.uniform(first, (total_rows, 1), jnp.float32, math.log(0.25), 0.0)) * ramp[:, None]
    base = jnp.abs(jax.random.normal(second, (total_rows, NEURONS), jnp.float32))
    keeper = jax.random.bernoulli(third, 0.5, (total_rows, NEURONS)).astype(jnp.float32)
    values = jnp.minimum(base * keeper * scales, 12.0)
    return values.astype(jnp.bfloat16)


def draw_block_index(key, part):
    blocks = NEURONS // TILE
    scores = jax.random.randint(key, (LAYERS, blocks, blocks), 0, 1 << 20, jnp.int32)
    scores = scores * blocks + jnp.arange(blocks, dtype=jnp.int32)
    picked = jax.lax.top_k(scores, K)[1]
    return picked.astype(jnp.int32)


def block_scale(own_key, dims, pieces, smallest, high):
    loudness = 1.0
    for position, parts in pieces:
        draws = jax.random.uniform(jax.random.fold_in(jax.random.fold_in(own_key, 6), position), (parts,), jnp.float32, smallest / len(pieces), high / len(pieces))
        loudness = loudness * jnp.repeat(jnp.exp(draws), dims[position] // parts).reshape((-1,) + (1,) * (len(dims) - 1 - position))
    return loudness


def gaussian(stream_key, dims, width, reach, shards=(), kind=jnp.bfloat16):
    array = width * jax.random.normal(stream_key, dims, jnp.float32)
    if shards:
        array = array * block_scale(stream_key, dims, shards, -0.22, 0.18)
    return jnp.clip(array, -reach, reach).astype(kind)


def setup_inputs(seed: int = 0) -> dict:
    splits = jax.random.split(jax.random.key(seed), 5)
    images = draw_images(jax.random.fold_in(splits[4], 71), 0)
    weights = gaussian(splits[1], (LAYERS, BLOCKS, K * TILE, TILE), (K * TILE // 2) ** -0.5, 0.375, ((1, 4),))
    block_index = draw_block_index(jax.random.fold_in(splits[4], 71), 0)
    bias = jnp.clip(jax.random.uniform(splits[3], (LAYERS, NEURONS), jnp.float32, -0.2, -0.02), -0.2, -0.02)
    return dict(images=images, weights=weights, block_index=block_index, bias=bias)


live_level = 0.25


def reference(images, weights, block_index, bias):
    blocks = NEURONS // TILE
    current = images
    live_terms = []
    for layer_no in range(LAYERS):
        tiles = weights[layer_no].astype(jnp.float32)
        chosen = block_index[layer_no].reshape(-1).astype(jnp.int32)
        offsets = bias[layer_no]

        def apply_layer(batch_rows):
            count = batch_rows.shape[0]
            blocked = batch_rows.reshape(count, blocks, TILE)
            picked = jnp.take(blocked, chosen, axis=1).reshape(count, blocks, K * TILE).astype(jnp.float32)
            result = jnp.einsum("brk,rkc->brc", picked, tiles, precision=lax.Precision.HIGHEST)
            result = result.reshape(count, NEURONS) + offsets
            return jnp.maximum(result, 0.0).astype(jnp.bfloat16)

        current = lax.map(apply_layer, current.reshape(N_IMG, IMG_GRP, NEURONS)).reshape(N_IMG * IMG_GRP, NEURONS)
        means = jnp.sum(current.astype(jnp.float32), axis=1) / NEURONS
        live_terms.append(jnp.sum(jnp.minimum(1.0, means / live_level)) / (N_IMG * IMG_GRP))
    return current, jnp.stack(live_terms)
```

```python
import functools

import jax
import jax.numpy as jnp
from jax import lax
from jax.experimental import pallas as pl
from jax.experimental.pallas import tpu as pltpu
from jax.sharding import PartitionSpec as P

live_level = 0.25


def xor_pairs(count, mask):
    return [(i, i ^ mask) for i in range(count)]


def layers_kernel(
    position_ref, shard_ref, column_ref, block_ref,
    own_ref, near_ref, far_ref, cross_ref, weights_ref, near_weights_ref, far_weights_ref, cross_weights_ref, bias_ref,
    mine_ref, theirs_ref, sums_ref,
    inputs, first, tiles, second_tiles, total, sems,
):
    position = position_ref[0]
    core = lax.rem(position, 2)
    half = near_ref.shape[0]
    rows, width = first.shape[0] // 4, first.shape[-1]
    deep = tiles.shape[1] // rows

    copies = []

    def fetch(source, target):
        copy = pltpu.make_async_copy(source, target, sems.at[len(copies)])
        copy.start()
        copies.append(copy)

    fetch(own_ref.at[pl.ds(pl.multiple_of(core * half, half), half), :], inputs.at[position])
    for mask, ref in ((1, near_ref), (2, far_ref), (3, cross_ref)):
        fetch(ref, inputs.at[position ^ mask])
    fetch(weights_ref.at[0], tiles.at[0])
    fetch(near_weights_ref.at[0], tiles.at[1])
    fetch(far_weights_ref, tiles.at[2])
    fetch(cross_weights_ref, tiles.at[3])
    fetch(weights_ref.at[1], second_tiles.at[0])
    fetch(near_weights_ref.at[1], second_tiles.at[1])

    for copy in copies[:4]:
        copy.wait()
    total[...] = jnp.zeros_like(total)
    for mask in range(4):
        copies[4 + mask].wait()
        start = (position ^ mask) * rows

        @pl.loop(0, rows, unroll=2)
        def _(r):
            row = start + r
            parts = []
            for k in range(4):
                column = pl.multiple_of(column_ref[row * 4 + k], width)
                parts.append(inputs[shard_ref[row * 4 + k], :, pl.ds(column, width)])
            tile = tiles[mask, pl.ds(pl.multiple_of(r * deep, deep), deep), :]
            result = jnp.dot(jnp.concatenate(parts, axis=1), tile, preferred_element_type=jnp.float32)
            result = jnp.maximum(result + bias_ref[pl.ds(row, 1), :], 0.0).astype(jnp.bfloat16)
            first[row] = result
            total[...] += result.astype(jnp.float32)

    ones = jnp.ones((8, width), jnp.float32)

    def collapse(value):
        return lax.dot_general(
            ones, value, (((1,), (1,)), ((), ())), precision=lax.Precision.HIGHEST, preferred_element_type=jnp.float32
        )

    sums_ref[0] = collapse(total[...])
    total[...] = jnp.zeros_like(total)
    for mask, out_ref in ((0, mine_ref), (1, theirs_ref)):
        copies[8 + mask].wait()
        start = (position ^ mask) * rows

        @pl.loop(0, rows, unroll=2)
        def _(r):
            row = start + r + 4 * rows
            parts = [first[block_ref[(start + r) * 4 + k]] for k in range(4)]
            tile = second_tiles[mask, pl.ds(pl.multiple_of(r * deep, deep), deep), :]
            result = jnp.dot(jnp.concatenate(parts, axis=1), tile, preferred_element_type=jnp.float32)
            result = jnp.maximum(result + bias_ref[pl.ds(row, 1), :], 0.0).astype(jnp.bfloat16)
            out_ref[:, pl.ds(pl.multiple_of(r * width, width), width)] = result
            total[...] += result.astype(jnp.float32)

    sums_ref[1] = collapse(total[...])


def per_device(images, weights, block_index, bias):
    layers, rows, deep, width = weights.shape
    count, shard = images.shape
    sides = lax.axis_size("nrn")
    groups = lax.axis_size("img")
    assert layers == 2 and sides == 4 and block_index.shape[-1] == 4
    neurons = shard * sides
    position = lax.axis_index("nrn")
    group = lax.axis_index("img")
    core = lax.rem(position, 2)
    half = count // 2
    nrn = functools.partial(lax.ppermute, axis_name="nrn")

    weights = weights.reshape(layers, rows * deep, width)
    piece_rows = rows * deep // groups
    piece = lax.dynamic_slice(weights, (0, group * piece_rows, 0), (1, piece_rows, width))[0]
    piece = nrn(piece, perm=xor_pairs(sides, 2))
    far_weights = lax.all_gather(piece, "img", axis=0, tiled=True)
    cross_weights = nrn(far_weights, perm=xor_pairs(sides, 1))
    near_weights = nrn(weights, perm=xor_pairs(sides, 1))

    kept = lax.dynamic_slice(images, (core * half, 0), (half, shard))
    given = lax.dynamic_slice(images, ((1 - core) * half, 0), (half, shard))
    far = nrn(kept, perm=xor_pairs(sides, 2))
    cross = nrn(given, perm=xor_pairs(sides, 3))
    near = nrn(given, perm=xor_pairs(sides, 1))

    any_space = pl.BlockSpec(memory_space=pl.ANY)
    smem = pl.BlockSpec(memory_space=pltpu.SMEM)
    vmem = pl.BlockSpec(memory_space=pltpu.VMEM)
    mine, theirs, sums = pl.pallas_call(
        layers_kernel,
        out_shape=(
            jax.ShapeDtypeStruct((half, shard), jnp.bfloat16),
            jax.ShapeDtypeStruct((half, shard), jnp.bfloat16),
            jax.ShapeDtypeStruct((layers, 8, half), jnp.float32),
        ),
        in_specs=[smem] * 4 + [any_space] * 8 + [vmem],
        out_specs=(vmem,) * 3,
        scratch_shapes=[
            pltpu.VMEM((sides, half, shard), jnp.bfloat16),
            pltpu.VMEM((sides * rows, half, width), jnp.bfloat16),
            pltpu.VMEM((sides, rows * deep, width), jnp.bfloat16),
            pltpu.VMEM((2, rows * deep, width), jnp.bfloat16),
            pltpu.VMEM((half, width), jnp.float32),
            pltpu.SemaphoreType.DMA((10,)),
        ],
        compiler_params=pltpu.CompilerParams(vmem_limit_bytes=60 * 2**20),
        cost_estimate=pl.CostEstimate(flops=12 * half * rows * deep * width, bytes_accessed=2**25, transcendentals=0),
    )(
        position.reshape(1), (block_index[0] // rows).reshape(-1), (block_index[0] % rows * width).reshape(-1), block_index[1].reshape(-1),
        images, near, far, cross, weights, near_weights, far_weights, cross_weights, bias.reshape(layers * sides * rows, width),
    )

    back = nrn(theirs, perm=xor_pairs(sides, 1))
    activations = jnp.where(core == 0, jnp.concatenate([mine, back]), jnp.concatenate([back, mine]))

    sums = sums[:, 0]
    second = sums[1] + nrn(sums[1], perm=xor_pairs(sides, 2))
    totals = jnp.stack([sums[0], second])
    live = jnp.sum(jnp.minimum(1.0, totals / neurons / live_level), axis=1)
    live = live + nrn(live, perm=xor_pairs(sides, 1))
    if groups & (groups - 1):
        live = lax.psum(live, "img")
    else:
        mask = 1
        while mask < groups:
            live = live + lax.ppermute(live, "img", xor_pairs(groups, mask))
            mask *= 2
    return activations, live / (count * groups)


def solution(mesh):
    in_specs = (P("img", "nrn"), P(None, "nrn", None, None), P(), P())
    out_specs = (P("img", "nrn"), P())
    return jax.shard_map(
        per_device, mesh=mesh, in_specs=in_specs, out_specs=out_specs, check_vma=False
    )
```

```python
import functools

import jax
import jax.numpy as jnp
from jax import lax
from jax.experimental import pallas as pl
from jax.experimental.pallas import tpu as pltpu
from jax.sharding import PartitionSpec as P


live_level = 0.25


def xor_pairs(count, mask):
    return [(i, i ^ mask) for i in range(count)]


def layers_kernel(
    layout, position_ref, place_ref, shard_ref, column_ref, block_ref, bias_ref,
    own_ref, near_ref, far_ref, cross_ref, weights_ref, near_weights_ref, *refs,
):
    piece_refs, refs = refs[: len(layout)], refs[len(layout) :]
    mine_ref, theirs_ref, sums_ref, inputs, first, tiles, second_tiles, total, sems = refs
    position = position_ref[0]
    core = lax.rem(position, 2)
    half = near_ref.shape[0]
    rows, width = first.shape[0] // 4, first.shape[-1]
    deep = tiles.shape[1] // rows

    copies = []

    def fetch(source, target):
        copy = pltpu.make_async_copy(source, target, sems.at[len(copies)])
        copy.start()
        copies.append(copy)

    fetch(own_ref.at[pl.ds(pl.multiple_of(core * half, half), half), :], inputs.at[position])
    for mask, ref in ((1, near_ref), (2, far_ref), (3, cross_ref)):
        fetch(ref, inputs.at[position ^ mask])
    fetch(weights_ref.at[0], tiles.at[0])
    fetch(near_weights_ref.at[0], tiles.at[1])
    fetch(weights_ref.at[1], second_tiles.at[0])
    fetch(near_weights_ref.at[1], second_tiles.at[1])

    def each_piece(slot, act):
        for i, (ref, own_slot) in enumerate(zip(piece_refs, layout)):
            if own_slot == slot:
                place = place_ref[i]

                @pl.when(place >= 0)
                def _():
                    target = tiles.at[slot, pl.ds(pl.multiple_of(place, 16), ref.shape[0])]
                    act(pltpu.make_async_copy(ref, target, sems.at[8 + i]))

    for slot in (2, 3):
        each_piece(slot, lambda copy: copy.start())

    for copy in copies[:4]:
        copy.wait()
    total[...] = jnp.zeros_like(total)
    for mask in range(4):
        if mask < 2:
            copies[4 + mask].wait()
        else:
            each_piece(mask, lambda copy: copy.wait())
        start = (position ^ mask) * rows

        @pl.loop(0, rows, unroll=16)
        def _(r):
            row = start + r
            parts = []
            for k in range(4):
                column = pl.multiple_of(column_ref[row * 4 + k], width)
                parts.append(inputs[shard_ref[row * 4 + k], :, pl.ds(column, width)])
            tile = tiles[mask, pl.ds(pl.multiple_of(r * deep, deep), deep), :]
            result = jnp.dot(jnp.concatenate(parts, axis=1), tile, preferred_element_type=jnp.float32)
            result = jnp.maximum(result + bias_ref[pl.ds(row, 1), :], 0.0).astype(jnp.bfloat16)
            first[row] = result
            total[...] += result.astype(jnp.float32)

    ones = jnp.ones((8, width), jnp.float32)

    def collapse(value):
        return lax.dot_general(
            ones, value, (((1,), (1,)), ((), ())), precision=lax.Precision.HIGHEST, preferred_element_type=jnp.float32
        )

    sums_ref[0] = collapse(total[...])
    total[...] = jnp.zeros_like(total)
    for mask, out_ref in ((0, mine_ref), (1, theirs_ref)):
        copies[6 + mask].wait()
        start = (position ^ mask) * rows

        @pl.loop(0, rows, unroll=16)
        def _(r):
            row = start + r + 4 * rows
            parts = [first[block_ref[(start + r) * 4 + k]] for k in range(4)]
            tile = second_tiles[mask, pl.ds(pl.multiple_of(r * deep, deep), deep), :]
            result = jnp.dot(jnp.concatenate(parts, axis=1), tile, preferred_element_type=jnp.float32)
            result = jnp.maximum(result + bias_ref[pl.ds(row, 1), :], 0.0).astype(jnp.bfloat16)
            out_ref[:, pl.ds(pl.multiple_of(r * width, width), width)] = result
            total[...] += result.astype(jnp.float32)

    sums_ref[1] = collapse(total[...])


def gather_far(weights, position, group, sides, groups):
    rows, width = weights.shape[1:]
    nrn = functools.partial(lax.ppermute, axis_name="nrn")
    both = functools.partial(lax.ppermute, axis_name=("img", "nrn"))
    piece_rows = rows // groups
    piece = lax.dynamic_slice(weights, (0, group * piece_rows, 0), (1, piece_rows, width))[0]
    piece = nrn(piece, perm=xor_pairs(sides, 2))
    if groups % 2 or groups > 8:
        far = lax.all_gather(piece, "img", axis=0, tiled=True)
        return [far, nrn(far, perm=xor_pairs(sides, 1))], [2, 3], jnp.zeros((2,), jnp.int32)

    line = groups // 2
    spot, side = group // 2, group % 2
    upward = lax.rem(position, 2) == 0

    def pairs(steps, move):
        found = []
        for g in range(groups):
            for n in range(sides):
                source = g // 2 - steps if n % 2 == 0 else g // 2 + steps
                target = move(g, n)
                if 0 <= source < line and 0 <= target[0] < groups:
                    found.append((g * sides + n, target[0] * sides + target[1]))
        return found

    def onward(g, n):
        return (g + 2 if n % 2 == 0 else g - 2), n

    def beside(g, n):
        return g ^ 1, n

    arrays, slots, places = [], [], []

    def keep(array, slot, steps, crossed, passed):
        step = jnp.where(upward != passed, -steps, steps)
        source = spot + step
        row = (source * 2 + (1 - side if crossed else side)) * piece_rows
        arrays.append(array)
        slots.append(slot)
        places.append(jnp.where((source >= 0) & (source < line), row, -1))

    held = [piece, nrn(piece, perm=xor_pairs(sides, 1))]
    keep(held[0], 2, 0, False, False)
    keep(held[1], 3, 0, False, False)
    other = both(piece, perm=pairs(0, beside))
    other_near = nrn(other, perm=xor_pairs(sides, 1))
    keep(other, 2, 0, True, False)
    keep(other_near, 3, 0, True, False)
    for s in range(1, line):
        for h in range(2):
            held[h] = both(held[h], perm=pairs(s - 1, onward))
            keep(held[h], 2 + h, s, False, False)
            keep(nrn(held[h], perm=xor_pairs(sides, 1)), 3 - h, s, False, True)
            other = both(held[h], perm=pairs(s, beside))
            keep(other, 2 + h, s, True, False)
            keep(nrn(other, perm=xor_pairs(sides, 1)), 3 - h, s, True, True)
    return arrays, slots, jnp.stack(places).astype(jnp.int32)


def per_device(images, weights, block_index, bias):
    layers, rows, deep, width = weights.shape
    count, shard = images.shape
    sides = lax.axis_size("nrn")
    groups = lax.axis_size("img")
    assert layers == 2 and sides == 4 and block_index.shape[-1] == 4
    neurons = shard * sides
    position = lax.axis_index("nrn")
    group = lax.axis_index("img")
    core = lax.rem(position, 2)
    half = count // 2
    nrn = functools.partial(lax.ppermute, axis_name="nrn")

    weights = weights.reshape(layers, rows * deep, width)
    pieces, layout, places = gather_far(weights, position, group, sides, groups)

    tables = (
        position.reshape(1), places, (block_index[0] // rows).reshape(-1), (block_index[0] % rows * width).reshape(-1),
        block_index[1].reshape(-1), bias.reshape(layers * sides * rows, width),
    )
    weights, tables = lax.optimization_barrier((weights, tables))
    near_weights = nrn(weights, perm=xor_pairs(sides, 1))
    kept = lax.dynamic_slice(images, (core * half, 0), (half, shard))
    given = lax.dynamic_slice(images, ((1 - core) * half, 0), (half, shard))
    far = nrn(kept, perm=xor_pairs(sides, 2))
    cross = nrn(given, perm=xor_pairs(sides, 3))
    near = nrn(given, perm=xor_pairs(sides, 1))

    any_space = pl.BlockSpec(memory_space=pl.ANY)
    smem = pl.BlockSpec(memory_space=pltpu.SMEM)
    vmem = pl.BlockSpec(memory_space=pltpu.VMEM)
    mine, theirs, sums = pl.pallas_call(
        functools.partial(layers_kernel, layout),
        out_shape=(
            jax.ShapeDtypeStruct((half, shard), jnp.bfloat16),
            jax.ShapeDtypeStruct((half, shard), jnp.bfloat16),
            jax.ShapeDtypeStruct((layers, 8, half), jnp.float32),
        ),
        in_specs=[smem] * 5 + [vmem] + [any_space] * (6 + len(pieces)),
        out_specs=(vmem,) * 3,
        scratch_shapes=[
            pltpu.VMEM((sides, half, shard), jnp.bfloat16),
            pltpu.VMEM((sides * rows, half, width), jnp.bfloat16),
            pltpu.VMEM((sides, rows * deep, width), jnp.bfloat16),
            pltpu.VMEM((2, rows * deep, width), jnp.bfloat16),
            pltpu.VMEM((half, width), jnp.float32),
            pltpu.SemaphoreType.DMA((8 + len(pieces),)),
        ],
        compiler_params=pltpu.CompilerParams(vmem_limit_bytes=60 * 2**20),
        cost_estimate=pl.CostEstimate(flops=12 * half * rows * deep * width, bytes_accessed=2**25, transcendentals=0),
    )(
        *tables, images, near, far, cross, weights, near_weights, *pieces,
    )

    back = nrn(theirs, perm=xor_pairs(sides, 1))
    activations = jnp.where(core == 0, jnp.concatenate([mine, back]), jnp.concatenate([back, mine]))

    sums = sums[:, 0]
    second = sums[1] + nrn(sums[1], perm=xor_pairs(sides, 2))
    totals = jnp.stack([sums[0], second])
    live = jnp.sum(jnp.minimum(1.0, totals / neurons / live_level), axis=1)
    live = live + nrn(live, perm=xor_pairs(sides, 1))
    if groups & (groups - 1):
        live = lax.psum(live, "img")
    else:
        mask = 1
        while mask < groups:
            live = live + lax.ppermute(live, "img", xor_pairs(groups, mask))
            mask *= 2
    return activations, live / (count * groups)


def solution(mesh):
    in_specs = (P("img", "nrn"), P(None, "nrn", None, None), P(), P())
    out_specs = (P("img", "nrn"), P())
    return jax.shard_map(
        per_device, mesh=mesh, in_specs=in_specs, out_specs=out_specs, check_vma=False
    )
```

```python
import functools

import jax
import jax.numpy as jnp
from jax import lax
from jax.experimental import pallas as pl
from jax.experimental.pallas import tpu as pltpu
from jax.sharding import PartitionSpec as P


live_level = 0.25


def xor_pairs(count, mask):
    return [(i, i ^ mask) for i in range(count)]


def layers_kernel(
    slots, position_ref, place_ref, block_ref, bias_ref,
    own_ref, near_ref, far_ref, cross_ref, weights_ref, near_weights_ref, *refs,
):
    piece_refs, refs = refs[: len(slots)], refs[len(slots) :]
    activations_ref, theirs_ref, sums_ref, second_sums_ref, inputs, first, tiles, second_tiles, outputs, sems = refs
    position = position_ref[0]
    core = lax.rem(position, 2)
    own_rows = pl.ds(pl.multiple_of(core * near_ref.shape[0], near_ref.shape[0]), near_ref.shape[0])
    sides = tiles.shape[0]
    blocks, half, width = first.shape
    rows = blocks // sides
    deep = tiles.shape[1] // rows

    sources = ((0, own_ref.at[own_rows]), (1, near_ref), (2, far_ref), (3, cross_ref))
    for mask, ref in sources:
        for r in range(rows):
            block = (position ^ mask) * rows + r
            pltpu.make_async_copy(ref.at[:, pl.ds(r * width, width)], inputs.at[block], sems.at[0]).start()
    loads = [
        pltpu.make_async_copy(ref.at[layer], target.at[mask], sems.at[1 + 2 * layer + mask])
        for layer, target in ((0, tiles), (1, second_tiles)) for mask, ref in ((0, weights_ref), (1, near_weights_ref))
    ]

    def each_piece(slot, act):
        for i, (ref, own_slot) in enumerate(zip(piece_refs, slots)):
            if own_slot == slot:
                place = place_ref[i]

                @pl.when(place >= 0)
                def _():
                    target = tiles.at[slot, pl.ds(pl.multiple_of(place, 16), ref.shape[0])]
                    act(pltpu.make_async_copy(ref, target, sems.at[7 + i]))

    for load in loads[:2]:
        load.start()
    for slot in (2, 3):
        each_piece(slot, lambda copy: copy.start())
    for load in loads[2:]:
        load.start()
    pltpu.make_async_copy(inputs, inputs, sems.at[0]).wait()

    def outcome(parts, tile, row):
        result = jnp.dot(jnp.concatenate(parts, axis=1), tile, preferred_element_type=jnp.float32)
        return jnp.maximum(result + bias_ref[pl.ds(row, 1), :], 0.0).astype(jnp.bfloat16)

    def first_layer(mask, total):
        for slot in range(sides):
            @pl.when(mask == slot)
            def _():
                if slot < 2:
                    loads[slot].wait()
                else:
                    each_piece(slot, lambda copy: copy.wait())

        for r in range(rows):
            row = (position ^ mask) * rows + r
            parts = [inputs[block_ref[row * 4 + k]] for k in range(4)]
            first[row] = result = outcome(parts, tiles[mask, r * deep : (r + 1) * deep, :], row)
            total = total + result.astype(jnp.float32)
        return total

    def second_layer(step, total):
        mask = 1 - step
        for slot in range(2):
            @pl.when(mask == slot)
            def _():
                loads[2 + slot].wait()

        for r in range(rows):
            row = (position ^ mask) * rows + r + blocks
            parts = [first[block_ref[row * 4 + k]] for k in range(4)]
            result = outcome(parts, second_tiles[mask, r * deep : (r + 1) * deep, :], row)
            outputs[mask, :, r * width : (r + 1) * width] = result
            total = total + result.astype(jnp.float32)

        @pl.when(mask == 1)
        def _():
            pltpu.make_async_copy(outputs.at[1], theirs_ref, sems.at[5]).start()

        return total

    ones = jnp.ones((8, width), jnp.float32)

    def collapse(value):
        return lax.dot_general(
            ones, value, (((1,), (1,)), ((), ())), precision=lax.Precision.HIGHEST, preferred_element_type=jnp.float32
        )

    zero = jnp.zeros((half, width), jnp.float32)
    sums_ref[...] = collapse(lax.fori_loop(0, sides, first_layer, zero))
    second_total = lax.fori_loop(0, 2, second_layer, zero)
    mine = pltpu.make_async_copy(outputs.at[0], activations_ref.at[own_rows], sems.at[6])
    mine.start()
    second_sums_ref[...] = collapse(second_total)
    pltpu.make_async_copy(outputs.at[1], theirs_ref, sems.at[5]).wait()
    mine.wait()


def gather_far(weights, position, group, sides, groups):
    rows, width = weights.shape[1:]
    nrn = functools.partial(lax.ppermute, axis_name="nrn")
    both = functools.partial(lax.ppermute, axis_name=("img", "nrn"))
    piece_rows = rows // groups
    splits = 2 if piece_rows % 32 == 0 else 1
    part_rows = piece_rows // splits
    parts = []
    for h in range(splits):
        part = lax.dynamic_slice(weights, (0, group * piece_rows + h * part_rows, 0), (1, part_rows, width))[0]
        parts.append(nrn(part, perm=xor_pairs(sides, 2)))
    if groups % 2 or groups > 8:
        piece = jnp.concatenate(parts)
        far = lax.all_gather(piece, "img", axis=0, tiled=True)
        return [far, nrn(far, perm=xor_pairs(sides, 1))], [2, 3], jnp.zeros((2,), jnp.int32)

    line = groups // 2
    spot, side = group // 2, group % 2
    upward = lax.rem(position, 2) == 0

    def pairs(steps, move):
        found = []
        for g in range(groups):
            for n in range(sides):
                source = g // 2 - steps if n % 2 == 0 else g // 2 + steps
                target = move(g, n)
                if 0 <= source < line and 0 <= target[0] < groups:
                    found.append((g * sides + n, target[0] * sides + target[1]))
        return found

    def onward(g, n):
        return (g + 2 if n % 2 == 0 else g - 2), n

    def beside(g, n):
        return g ^ 1, n

    arrays, slots, places = [], [], []

    def keep(array, slot, steps, crossed, passed, offset=0):
        step = jnp.where(upward != passed, -steps, steps)
        source = spot + step
        row = (source * 2 + (1 - side if crossed else side)) * piece_rows + offset
        arrays.append(array)
        slots.append(slot)
        places.append(jnp.where((source >= 0) & (source < line), row, -1))

    for h, part in enumerate(parts):
        other = both(part, perm=pairs(0, beside))
        keep(other, 2, 0, True, False, h * part_rows)
        keep(nrn(other, perm=xor_pairs(sides, 1)), 3, 0, True, False, h * part_rows)
    piece = jnp.concatenate(parts)
    held = [piece, nrn(piece, perm=xor_pairs(sides, 1))]
    keep(held[0], 2, 0, False, False)
    keep(held[1], 3, 0, False, False)
    for s in range(1, line):
        for h in range(2):
            held[h] = both(held[h], perm=pairs(s - 1, onward))
            keep(held[h], 2 + h, s, False, False)
            keep(nrn(held[h], perm=xor_pairs(sides, 1)), 3 - h, s, False, True)
            other = both(held[h], perm=pairs(s, beside))
            keep(other, 2 + h, s, True, False)
            keep(nrn(other, perm=xor_pairs(sides, 1)), 3 - h, s, True, True)
    return arrays, slots, jnp.stack(places).astype(jnp.int32)


def per_device(images, weights, block_index, bias):
    layers, rows, deep, width = weights.shape
    count, shard = images.shape
    sides = lax.axis_size("nrn")
    groups = lax.axis_size("img")
    assert layers == 2 and sides == 4 and block_index.shape[-1] == 4
    neurons = shard * sides
    position = lax.axis_index("nrn")
    group = lax.axis_index("img")
    core = lax.rem(position, 2)
    half = count // 2
    nrn = functools.partial(lax.ppermute, axis_name="nrn")

    weights = weights.reshape(layers, rows * deep, width)
    pieces, slots, places = gather_far(weights, position, group, sides, groups)

    kept = lax.dynamic_slice(images, (core * half, 0), (half, shard))
    given = lax.dynamic_slice(images, ((1 - core) * half, 0), (half, shard))
    far = nrn(kept, perm=xor_pairs(sides, 2))
    cross = nrn(given, perm=xor_pairs(sides, 3))
    tables = position.reshape(1), places, block_index.reshape(-1), bias.reshape(layers * sides * rows, width)
    given, tables = lax.optimization_barrier((given, tables))
    near = nrn(given, perm=xor_pairs(sides, 1))
    near_weights = nrn(weights, perm=xor_pairs(sides, 1))

    any_space = pl.BlockSpec(memory_space=pl.ANY)
    smem = pl.BlockSpec(memory_space=pltpu.SMEM)
    vmem = pl.BlockSpec(memory_space=pltpu.VMEM)
    activations, theirs, first_sums, second_sums = pl.pallas_call(
        functools.partial(layers_kernel, slots),
        out_shape=(
            jax.ShapeDtypeStruct((count, shard), jnp.bfloat16),
            jax.ShapeDtypeStruct((half, shard), jnp.bfloat16),
            jax.ShapeDtypeStruct((8, half), jnp.float32),
            jax.ShapeDtypeStruct((8, half), jnp.float32),
        ),
        in_specs=[smem] * 3 + [vmem] + [any_space] * (6 + len(pieces)),
        out_specs=(any_space, any_space, vmem, vmem),
        scratch_shapes=[
            pltpu.VMEM((sides * rows, half, width), jnp.bfloat16),
            pltpu.VMEM((sides * rows, half, width), jnp.bfloat16),
            pltpu.VMEM((sides, rows * deep, width), jnp.bfloat16),
            pltpu.VMEM((2, rows * deep, width), jnp.bfloat16),
            pltpu.VMEM((2, half, shard), jnp.bfloat16),
            pltpu.SemaphoreType.DMA((7 + len(pieces),)),
        ],
        compiler_params=pltpu.CompilerParams(vmem_limit_bytes=36 * 2**20),
        cost_estimate=pl.CostEstimate(flops=12 * half * rows * deep * width, bytes_accessed=2**25, transcendentals=0),
    )(*tables, images, near, far, cross, weights, near_weights, *pieces)

    back = nrn(theirs, perm=xor_pairs(sides, 1))
    activations = lax.dynamic_update_slice(activations, back, ((1 - core) * half, 0))

    second_sums = second_sums + nrn(second_sums, perm=xor_pairs(sides, 2))
    totals = jnp.stack([first_sums[0], second_sums[0]])
    live = jnp.sum(jnp.minimum(1.0, totals / neurons / live_level), axis=1)
    if groups & (groups - 1):
        live = live + nrn(live, perm=xor_pairs(sides, 1))
        live = lax.psum(live, "img")
    else:
        live = live + nrn(live, perm=xor_pairs(sides, 1))
        mask = 1
        while mask < groups:
            live = live + lax.ppermute(live, "img", xor_pairs(groups, mask))
            mask *= 2
    return activations, live / (count * groups)


def solution(mesh):
    in_specs = (P("img", "nrn"), P(None, "nrn", None, None), P(), P())
    out_specs = (P("img", "nrn"), P())
    return jax.shard_map(
        per_device, mesh=mesh, in_specs=in_specs, out_specs=out_specs, check_vma=False
    )
```

```python
import functools

import jax
import jax.numpy as jnp
from jax import lax
from jax.experimental import pallas as pl
from jax.experimental.pallas import tpu as pltpu
from jax.sharding import PartitionSpec as P


live_level = 0.25
near_limit = 36 * 2**20
far_limit = 32 * 2**20


def xor_pairs(count, mask):
    return [(i, i ^ mask) for i in range(count)]


def outcome(parts, tile, bias):
    result = jnp.dot(jnp.concatenate(parts, axis=1), tile, preferred_element_type=jnp.float32)
    return jnp.maximum(result + bias, 0.0).astype(jnp.bfloat16)


def collapse(value):
    ones = jnp.ones((8, value.shape[1]), jnp.float32)
    return lax.dot_general(
        ones, value, (((1,), (1,)), ((), ())), precision=lax.Precision.HIGHEST, preferred_element_type=jnp.float32
    )


def near_kernel(
    position_ref, block_ref, bias_ref, own_ref, near_ref, far_ref, cross_ref, weights_ref, near_weights_ref,
    inputs, first, total_ref, tiles, sems,
):
    position = position_ref[0]
    core = lax.rem(position, 2)
    half = near_ref.shape[0]
    slots, rows, _, width = first.shape
    deep = tiles.shape[1] // rows
    own_rows = pl.ds(pl.multiple_of(core * half, half), half)
    for mask, ref in ((0, own_ref.at[own_rows]), (1, near_ref), (2, far_ref), (3, cross_ref)):
        for r in range(rows):
            block = (position ^ mask) * rows + r
            pltpu.make_async_copy(ref.at[:, pl.ds(r * width, width)], inputs.at[block], sems.at[0]).start()
    loads = [
        pltpu.make_async_copy(ref.at[0], tiles.at[mask], sems.at[1 + mask])
        for mask, ref in enumerate((weights_ref, near_weights_ref))
    ]
    for load in loads:
        load.start()
    pltpu.make_async_copy(inputs, inputs, sems.at[0]).wait()

    def layer(mask, total):
        for slot in range(slots):
            @pl.when(mask == slot)
            def _():
                loads[slot].wait()

        for r in range(rows):
            row = (position ^ mask) * rows + r
            parts = [inputs[block_ref[row * 4 + k]] for k in range(4)]
            first[mask, r] = result = outcome(parts, tiles[mask, r * deep : (r + 1) * deep, :], bias_ref[pl.ds(row, 1), :])
            total = total + result.astype(jnp.float32)
        return total

    total_ref[...] = lax.fori_loop(0, slots, layer, jnp.zeros((half, width), jnp.float32))


def far_kernel(
    slots, position_ref, place_ref, block_ref, bias_ref, inputs, near_first, total_ref, weights_ref, near_weights_ref, *refs,
):
    piece_refs, refs = refs[: len(slots)], refs[len(slots) :]
    activations_ref, theirs_ref, sums_ref, second_sums_ref, first, tiles, second_tiles, outputs, sems = refs
    position = position_ref[0]
    core = lax.rem(position, 2)
    blocks, half, width = first.shape
    rows = near_first.shape[1]
    deep = tiles.shape[1] // rows

    def each_piece(slot, act):
        for i, (ref, own_slot) in enumerate(zip(piece_refs, slots)):
            if own_slot == slot:
                place = place_ref[i]

                @pl.when(place >= 0)
                def _():
                    target = tiles.at[slot - 2, pl.ds(pl.multiple_of(place, 16), ref.shape[0])]
                    act(pltpu.make_async_copy(ref, target, sems.at[6 + i]))

    loads = [
        pltpu.make_async_copy(ref.at[1], second_tiles.at[mask], sems.at[mask])
        for mask, ref in enumerate((weights_ref, near_weights_ref))
    ]
    moves = [
        pltpu.make_async_copy(
            near_first.at[mask], first.at[pl.ds(pl.multiple_of((position ^ mask) * rows, rows), rows)], sems.at[2 + mask]
        )
        for mask in range(2)
    ]
    for slot in (2, 3):
        each_piece(slot, lambda copy: copy.start())
    for copy in loads + moves:
        copy.start()

    def first_layer(step, total):
        for slot in (2, 3):
            @pl.when(step == slot - 2)
            def _():
                each_piece(slot, lambda copy: copy.wait())

        for r in range(rows):
            row = (position ^ (step + 2)) * rows + r
            parts = [inputs[block_ref[row * 4 + k]] for k in range(4)]
            first[row] = result = outcome(parts, tiles[step, r * deep : (r + 1) * deep, :], bias_ref[pl.ds(row, 1), :])
            total = total + result.astype(jnp.float32)
        return total

    sums_ref[...] = collapse(lax.fori_loop(0, 2, first_layer, total_ref[...]))
    for move in moves:
        move.wait()

    def second_layer(step, total):
        mask = 1 - step
        for slot in range(2):
            @pl.when(mask == slot)
            def _():
                loads[slot].wait()

        for r in range(rows):
            row = (position ^ mask) * rows + r + blocks
            parts = [first[block_ref[row * 4 + k]] for k in range(4)]
            result = outcome(parts, second_tiles[mask, r * deep : (r + 1) * deep, :], bias_ref[pl.ds(row, 1), :])
            outputs[mask, :, r * width : (r + 1) * width] = result
            total = total + result.astype(jnp.float32)

        @pl.when(mask == 1)
        def _():
            pltpu.make_async_copy(outputs.at[1], theirs_ref, sems.at[4]).start()

        return total

    second_total = lax.fori_loop(0, 2, second_layer, jnp.zeros((half, width), jnp.float32))
    own_rows = pl.ds(pl.multiple_of(core * half, half), half)
    mine = pltpu.make_async_copy(outputs.at[0], activations_ref.at[own_rows], sems.at[5])
    mine.start()
    second_sums_ref[...] = collapse(second_total)
    pltpu.make_async_copy(outputs.at[1], theirs_ref, sems.at[4]).wait()
    mine.wait()


def gather_far(weights, position, group, sides, groups):
    rows, width = weights.shape[1:]
    nrn = functools.partial(lax.ppermute, axis_name="nrn")
    both = functools.partial(lax.ppermute, axis_name=("img", "nrn"))
    piece_rows = rows // groups
    splits = 2 if piece_rows % 32 == 0 else 1
    part_rows = piece_rows // splits
    parts = []
    for h in range(splits):
        part = lax.dynamic_slice(weights, (0, group * piece_rows + h * part_rows, 0), (1, part_rows, width))[0]
        parts.append(nrn(part, perm=xor_pairs(sides, 2)))
    if groups % 2 or groups > 8:
        piece = jnp.concatenate(parts)
        far = lax.all_gather(piece, "img", axis=0, tiled=True)
        return [far, nrn(far, perm=xor_pairs(sides, 1))], [2, 3], jnp.zeros((2,), jnp.int32)

    line = groups // 2
    spot, side = group // 2, group % 2
    upward = lax.rem(position, 2) == 0

    def pairs(steps, move):
        found = []
        for g in range(groups):
            for n in range(sides):
                source = g // 2 - steps if n % 2 == 0 else g // 2 + steps
                target = move(g, n)
                if 0 <= source < line and 0 <= target[0] < groups:
                    found.append((g * sides + n, target[0] * sides + target[1]))
        return found

    def onward(g, n):
        return (g + 2 if n % 2 == 0 else g - 2), n

    def beside(g, n):
        return g ^ 1, n

    arrays, slots, places = [], [], []

    def keep(array, slot, steps, crossed, passed, offset=0):
        step = jnp.where(upward != passed, -steps, steps)
        source = spot + step
        row = (source * 2 + (1 - side if crossed else side)) * piece_rows + offset
        arrays.append(array)
        slots.append(slot)
        places.append(jnp.where((source >= 0) & (source < line), row, -1))

    for h, part in enumerate(parts):
        other = both(part, perm=pairs(0, beside))
        keep(other, 2, 0, True, False, h * part_rows)
        keep(nrn(other, perm=xor_pairs(sides, 1)), 3, 0, True, False, h * part_rows)
    piece = jnp.concatenate(parts)
    held = [piece, nrn(piece, perm=xor_pairs(sides, 1))]
    keep(held[0], 2, 0, False, False)
    keep(held[1], 3, 0, False, False)
    for s in range(1, line):
        for h in range(2):
            held[h] = both(held[h], perm=pairs(s - 1, onward))
            keep(held[h], 2 + h, s, False, False)
            keep(nrn(held[h], perm=xor_pairs(sides, 1)), 3 - h, s, False, True)
            other = both(held[h], perm=pairs(s, beside))
            keep(other, 2 + h, s, True, False)
            keep(nrn(other, perm=xor_pairs(sides, 1)), 3 - h, s, True, True)
    return arrays, slots, jnp.stack(places).astype(jnp.int32)


def per_device(images, weights, block_index, bias):
    layers, rows, deep, width = weights.shape
    count, shard = images.shape
    sides = lax.axis_size("nrn")
    groups = lax.axis_size("img")
    assert layers == 2 and sides == 4 and block_index.shape[-1] == 4
    neurons = shard * sides
    position = lax.axis_index("nrn")
    group = lax.axis_index("img")
    core = lax.rem(position, 2)
    half = count // 2
    nrn = functools.partial(lax.ppermute, axis_name="nrn")

    weights = weights.reshape(layers, rows * deep, width)
    pieces, slots, places = gather_far(weights, position, group, sides, groups)

    kept = lax.dynamic_slice(images, (core * half, 0), (half, shard))
    given = lax.dynamic_slice(images, ((1 - core) * half, 0), (half, shard))
    far = nrn(kept, perm=xor_pairs(sides, 2))
    cross = nrn(given, perm=xor_pairs(sides, 3))
    tables = position.reshape(1), places, block_index.reshape(-1), bias.reshape(layers * sides * rows, width)
    given, (place, places, blocks, biases) = lax.optimization_barrier((given, tables))
    near = nrn(given, perm=xor_pairs(sides, 1))
    near_weights = nrn(weights, perm=xor_pairs(sides, 1))

    any_space = pl.BlockSpec(memory_space=pl.ANY)
    smem = pl.BlockSpec(memory_space=pltpu.SMEM)
    vmem = pl.BlockSpec(memory_space=pltpu.VMEM)
    flops = 2 * half * rows * deep * width
    inputs, near_first, total = pl.pallas_call(
        near_kernel,
        out_shape=(
            jax.ShapeDtypeStruct((sides * rows, half, width), jnp.bfloat16),
            jax.ShapeDtypeStruct((2, rows, half, width), jnp.bfloat16),
            jax.ShapeDtypeStruct((half, width), jnp.float32),
        ),
        in_specs=[smem] * 2 + [vmem] + [any_space] * 6,
        out_specs=(vmem,) * 3,
        scratch_shapes=[pltpu.VMEM((2, rows * deep, width), jnp.bfloat16), pltpu.SemaphoreType.DMA((3,))],
        compiler_params=pltpu.CompilerParams(vmem_limit_bytes=near_limit),
        cost_estimate=pl.CostEstimate(flops=2 * flops, bytes_accessed=2**24, transcendentals=0),
    )(place, blocks, biases, images, near, far, cross, weights, near_weights)
    activations, theirs, first_sums, second_sums = pl.pallas_call(
        functools.partial(far_kernel, slots),
        out_shape=(
            jax.ShapeDtypeStruct((count, shard), jnp.bfloat16),
            jax.ShapeDtypeStruct((half, shard), jnp.bfloat16),
            jax.ShapeDtypeStruct((8, half), jnp.float32),
            jax.ShapeDtypeStruct((8, half), jnp.float32),
        ),
        in_specs=[smem] * 3 + [vmem] * 4 + [any_space] * (2 + len(pieces)),
        out_specs=(any_space, any_space, vmem, vmem),
        scratch_shapes=[
            pltpu.VMEM((sides * rows, half, width), jnp.bfloat16),
            pltpu.VMEM((2, rows * deep, width), jnp.bfloat16),
            pltpu.VMEM((2, rows * deep, width), jnp.bfloat16),
            pltpu.VMEM((2, half, shard), jnp.bfloat16),
            pltpu.SemaphoreType.DMA((6 + len(pieces),)),
        ],
        compiler_params=pltpu.CompilerParams(vmem_limit_bytes=far_limit),
        cost_estimate=pl.CostEstimate(flops=4 * flops, bytes_accessed=2**24, transcendentals=0),
    )(place, places, blocks, biases, inputs, near_first, total, weights, near_weights, *pieces)

    back = nrn(theirs, perm=xor_pairs(sides, 1))
    activations = lax.dynamic_update_slice(activations, back, ((1 - core) * half, 0))

    second_sums = second_sums + nrn(second_sums, perm=xor_pairs(sides, 2))
    totals = jnp.stack([first_sums[0], second_sums[0]])
    live = jnp.sum(jnp.minimum(1.0, totals / neurons / live_level), axis=1)
    if groups & (groups - 1):
        live = live + nrn(live, perm=xor_pairs(sides, 1))
        live = lax.psum(live, "img")
    else:
        live = live + nrn(live, perm=xor_pairs(sides, 1))
        mask = 1
        while mask < groups:
            live = live + lax.ppermute(live, "img", xor_pairs(groups, mask))
            mask *= 2
    return activations, live / (count * groups)


def solution(mesh):
    in_specs = (P("img", "nrn"), P(None, "nrn", None, None), P(), P())
    out_specs = (P("img", "nrn"), P())
    return jax.shard_map(
        per_device, mesh=mesh, in_specs=in_specs, out_specs=out_specs, check_vma=False
    )
```

```python
import functools

import jax
import jax.numpy as jnp
from jax import lax
from jax.experimental import pallas as pl
from jax.experimental.pallas import tpu as pltpu
from jax.sharding import PartitionSpec as P


live_level = 0.25
near_limit = 36 * 2**20
far_limit = 32 * 2**20


def xor_pairs(count, mask):
    return [(i, i ^ mask) for i in range(count)]


def outcome(parts, tile, bias):
    result = jnp.dot(jnp.concatenate(parts, axis=1), tile, preferred_element_type=jnp.float32)
    return jnp.maximum(result + bias, 0.0).astype(jnp.bfloat16)


def collapse(value):
    ones = jnp.ones((8, value.shape[1]), jnp.float32)
    return lax.dot_general(
        ones, value, (((1,), (1,)), ((), ())), precision=lax.Precision.HIGHEST, preferred_element_type=jnp.float32
    )


def near_kernel(
    position_ref, block_ref, bias_ref, own_ref, near_ref, far_ref, cross_ref, weights_ref, near_weights_ref,
    inputs, first, total_ref, tiles, sems,
):
    position = position_ref[0]
    core = lax.rem(position, 2)
    half = near_ref.shape[0]
    slots, rows, _, width = first.shape
    deep = tiles.shape[1] // rows
    own_rows = pl.ds(pl.multiple_of(core * half, half), half)
    for mask, ref in ((0, own_ref.at[own_rows]), (1, near_ref), (2, far_ref), (3, cross_ref)):
        for r in range(rows):
            block = (position ^ mask) * rows + r
            pltpu.make_async_copy(ref.at[:, pl.ds(r * width, width)], inputs.at[block], sems.at[0]).start()
    loads = [
        pltpu.make_async_copy(ref.at[0], tiles.at[mask], sems.at[1 + mask])
        for mask, ref in enumerate((weights_ref, near_weights_ref))
    ]
    for load in loads:
        load.start()
    pltpu.make_async_copy(inputs, inputs, sems.at[0]).wait()

    def layer(mask, total):
        for slot in range(slots):
            @pl.when(mask == slot)
            def _():
                loads[slot].wait()

        for r in range(rows):
            row = (position ^ mask) * rows + r
            parts = [inputs[block_ref[row * 4 + k]] for k in range(4)]
            first[mask, r] = result = outcome(parts, tiles[mask, r * deep : (r + 1) * deep, :], bias_ref[pl.ds(row, 1), :])
            total = total + result.astype(jnp.float32)
        return total

    total_ref[...] = lax.fori_loop(0, slots, layer, jnp.zeros((half, width), jnp.float32))


def far_kernel(
    slots, position_ref, place_ref, block_ref, bias_ref, inputs, near_first, total_ref, weights_ref, near_weights_ref, *refs,
):
    piece_refs, refs = refs[: len(slots)], refs[len(slots) :]
    activations_ref, theirs_ref, sums_ref, first, tiles, second_tiles, outputs, sems = refs
    position = position_ref[0]
    core = lax.rem(position, 2)
    blocks, half, width = first.shape
    rows = near_first.shape[1]
    deep = tiles.shape[1] // rows

    def each_piece(slot, act):
        for i, (ref, own_slot) in enumerate(zip(piece_refs, slots)):
            if own_slot == slot:
                place = place_ref[i]

                @pl.when(place >= 0)
                def _():
                    target = tiles.at[slot - 2, pl.ds(pl.multiple_of(place, 16), ref.shape[0])]
                    act(pltpu.make_async_copy(ref, target, sems.at[6 + i]))

    loads = [
        pltpu.make_async_copy(ref.at[1], second_tiles.at[mask], sems.at[mask])
        for mask, ref in enumerate((weights_ref, near_weights_ref))
    ]
    moves = [
        pltpu.make_async_copy(
            near_first.at[mask], first.at[pl.ds(pl.multiple_of((position ^ mask) * rows, rows), rows)], sems.at[2 + mask]
        )
        for mask in range(2)
    ]
    for slot in (2, 3):
        each_piece(slot, lambda copy: copy.start())
    for copy in loads + moves:
        copy.start()

    def first_layer(step, total):
        for slot in (2, 3):
            @pl.when(step == slot - 2)
            def _():
                each_piece(slot, lambda copy: copy.wait())

        for r in range(rows):
            row = (position ^ (step + 2)) * rows + r
            parts = [inputs[block_ref[row * 4 + k]] for k in range(4)]
            first[row] = result = outcome(parts, tiles[step, r * deep : (r + 1) * deep, :], bias_ref[pl.ds(row, 1), :])
            total = total + result.astype(jnp.float32)
        return total

    sums_ref[0] = collapse(lax.fori_loop(0, 2, first_layer, total_ref[...]))
    for move in moves:
        move.wait()

    def second_layer(step, total):
        mask = 1 - step
        for slot in range(2):
            @pl.when(mask == slot)
            def _():
                loads[slot].wait()

        for r in range(rows):
            row = (position ^ mask) * rows + r + blocks
            parts = [first[block_ref[row * 4 + k]] for k in range(4)]
            result = outcome(parts, second_tiles[mask, r * deep : (r + 1) * deep, :], bias_ref[pl.ds(row, 1), :])
            outputs[mask, :, r * width : (r + 1) * width] = result
            total = total + result.astype(jnp.float32)

        @pl.when(mask == 1)
        def _():
            pltpu.make_async_copy(outputs.at[1], theirs_ref, sems.at[4]).start()

        return total

    second_total = lax.fori_loop(0, 2, second_layer, jnp.zeros((half, width), jnp.float32))
    own_rows = pl.ds(pl.multiple_of(core * half, half), half)
    mine = pltpu.make_async_copy(outputs.at[0], activations_ref.at[own_rows], sems.at[5])
    mine.start()
    sums_ref[1] = collapse(second_total)
    pltpu.make_async_copy(outputs.at[1], theirs_ref, sems.at[4]).wait()
    mine.wait()


def gather_far(weights, position, group, sides, groups):
    rows, width = weights.shape[1:]
    nrn = functools.partial(lax.ppermute, axis_name="nrn")
    both = functools.partial(lax.ppermute, axis_name=("img", "nrn"))
    piece_rows = rows // groups
    splits = 2 if piece_rows % 32 == 0 else 1
    part_rows = piece_rows // splits
    parts = []
    for h in range(splits):
        part = lax.dynamic_slice(weights, (0, group * piece_rows + h * part_rows, 0), (1, part_rows, width))[0]
        parts.append(nrn(part, perm=xor_pairs(sides, 2)))
    if groups % 2 or groups > 8:
        piece = jnp.concatenate(parts)
        far = lax.all_gather(piece, "img", axis=0, tiled=True)
        return [far, nrn(far, perm=xor_pairs(sides, 1))], [2, 3], jnp.zeros((2,), jnp.int32), piece

    line = groups // 2
    spot, side = group // 2, group % 2
    upward = lax.rem(position, 2) == 0

    def far_end(z):
        return line - 1 if 2 * z < line else 0

    def pairs(steps, move, direct=False):
        found = []
        for g in range(groups):
            for n in range(sides):
                source = g // 2 - steps if n % 2 == 0 else g // 2 + steps
                target = move(g, n)
                if 0 <= source < line and 0 <= target[0] < groups and not (direct and source == far_end(g // 2)):
                    found.append((g * sides + n, target[0] * sides + target[1]))
        return found

    def onward(g, n):
        return (g + 2 if n % 2 == 0 else g - 2), n

    def beside(g, n):
        return g ^ 1, n

    arrays, slots, places = [], [], []

    last = jnp.where(2 * spot < line, line - 1, 0)

    def keep(array, slot, steps, crossed, passed, offset=0, direct=False):
        step = jnp.where(upward != passed, -steps, steps)
        source = spot + step
        row = (source * 2 + (1 - side if crossed else side)) * piece_rows + offset
        came = (source >= 0) & (source < line)
        if direct:
            came = came & (source != last)
        arrays.append(array)
        slots.append(slot)
        places.append(jnp.where(came, row, -1))

    last_row = (last * 2 + 1 - side) * piece_rows
    extra = lax.dynamic_slice(weights, (0, last_row, 0), (1, piece_rows, width))[0]
    extra = both(extra, perm=[
        (g * sides + n, g * sides + (n ^ 2)) for g in range(groups) for n in range(sides) if (n % 2 == 0) == (g < line)
    ])
    extra_near = nrn(extra, perm=xor_pairs(sides, 1))
    for slot, array, here in ((2, extra, upward), (3, extra_near, ~upward)):
        arrays.append(array)
        slots.append(slot)
        places.append(jnp.where(here == (2 * spot < line), last_row, -1))

    for h, part in enumerate(parts):
        other = both(part, perm=pairs(0, beside))
        keep(other, 2, 0, True, False, h * part_rows)
        keep(nrn(other, perm=xor_pairs(sides, 1)), 3, 0, True, False, h * part_rows)
    piece = jnp.concatenate(parts)
    held = [piece, nrn(piece, perm=xor_pairs(sides, 1))]
    keep(held[0], 2, 0, False, False)
    keep(held[1], 3, 0, False, False)
    for s in range(1, line):
        for h in range(2):
            held[h] = both(held[h], perm=pairs(s - 1, onward))
            keep(held[h], 2 + h, s, False, False)
            keep(nrn(held[h], perm=xor_pairs(sides, 1)), 3 - h, s, False, True)
            moves = pairs(s, beside, direct=h == 1)
            if not moves:
                continue
            other = both(held[h], perm=moves)
            keep(other, 2 + h, s, True, False, direct=h == 1)
            keep(nrn(other, perm=xor_pairs(sides, 1)), 3 - h, s, True, True, direct=h == 1)
    return arrays, slots, jnp.stack(places).astype(jnp.int32), parts[0]


def per_device(images, weights, block_index, bias):
    layers, rows, deep, width = weights.shape
    count, shard = images.shape
    sides = lax.axis_size("nrn")
    groups = lax.axis_size("img")
    assert layers == 2 and sides == 4 and block_index.shape[-1] == 4
    neurons = shard * sides
    position = lax.axis_index("nrn")
    group = lax.axis_index("img")
    core = lax.rem(position, 2)
    half = count // 2
    nrn = functools.partial(lax.ppermute, axis_name="nrn")

    weights = weights.reshape(layers, rows * deep, width)
    pieces, slots, places, arrived = gather_far(weights, position, group, sides, groups)

    tables = position.reshape(1), places, block_index.reshape(-1), bias.reshape(layers * sides * rows, width)
    sent_weights, (place, places, blocks, biases) = lax.optimization_barrier((weights, tables))
    near_weights = nrn(sent_weights, perm=xor_pairs(sides, 1))
    kept = lax.dynamic_slice(images, (core * half, 0), (half, shard))
    far = nrn(kept, perm=xor_pairs(sides, 2))
    late_images, _ = lax.optimization_barrier((images, arrived))
    given = lax.dynamic_slice(late_images, ((1 - core) * half, 0), (half, shard))
    cross = nrn(given, perm=xor_pairs(sides, 3))
    near = nrn(given, perm=xor_pairs(sides, 1))

    any_space = pl.BlockSpec(memory_space=pl.ANY)
    smem = pl.BlockSpec(memory_space=pltpu.SMEM)
    vmem = pl.BlockSpec(memory_space=pltpu.VMEM)
    flops = 2 * half * rows * deep * width
    inputs, near_first, total = pl.pallas_call(
        near_kernel,
        out_shape=(
            jax.ShapeDtypeStruct((sides * rows, half, width), jnp.bfloat16),
            jax.ShapeDtypeStruct((2, rows, half, width), jnp.bfloat16),
            jax.ShapeDtypeStruct((half, width), jnp.float32),
        ),
        in_specs=[smem] * 2 + [vmem] + [any_space] * 6,
        out_specs=(vmem,) * 3,
        scratch_shapes=[pltpu.VMEM((2, rows * deep, width), jnp.bfloat16), pltpu.SemaphoreType.DMA((3,))],
        compiler_params=pltpu.CompilerParams(vmem_limit_bytes=near_limit),
        cost_estimate=pl.CostEstimate(flops=2 * flops, bytes_accessed=2**24, transcendentals=0),
    )(place, blocks, biases, images, near, far, cross, weights, near_weights)
    activations, theirs, sums = pl.pallas_call(
        functools.partial(far_kernel, slots),
        out_shape=(
            jax.ShapeDtypeStruct((count, shard), jnp.bfloat16),
            jax.ShapeDtypeStruct((half, shard), jnp.bfloat16),
            jax.ShapeDtypeStruct((layers, 8, half), jnp.float32),
        ),
        in_specs=[smem] * 3 + [vmem] * 4 + [any_space] * (2 + len(pieces)),
        out_specs=(any_space, any_space, vmem),
        scratch_shapes=[
            pltpu.VMEM((sides * rows, half, width), jnp.bfloat16),
            pltpu.VMEM((2, rows * deep, width), jnp.bfloat16),
            pltpu.VMEM((2, rows * deep, width), jnp.bfloat16),
            pltpu.VMEM((2, half, shard), jnp.bfloat16),
            pltpu.SemaphoreType.DMA((6 + len(pieces),)),
        ],
        compiler_params=pltpu.CompilerParams(vmem_limit_bytes=far_limit),
        cost_estimate=pl.CostEstimate(flops=4 * flops, bytes_accessed=2**24, transcendentals=0),
    )(place, places, blocks, biases, inputs, near_first, total, weights, near_weights, *pieces)

    back = nrn(theirs, perm=xor_pairs(sides, 1))
    activations = lax.dynamic_update_slice(activations, back, ((1 - core) * half, 0))

    held = [sums]
    for mask in range(1, sides):
        held.append(nrn(sums, perm=xor_pairs(sides, mask)))
    totals = jnp.stack([
        jnp.stack([held[core_mask][0, 0], held[core_mask][1, 0] + held[core_mask ^ 2][1, 0]]) for core_mask in range(2)
    ])
    live = jnp.sum(jnp.minimum(1.0, totals / neurons / live_level), axis=(0, 2))
    if groups & (groups - 1):
        live = lax.psum(live, "img")
    else:
        mask = 1
        while mask < groups:
            live = live + lax.ppermute(live, "img", xor_pairs(groups, mask))
            mask *= 2
    return activations, live / (count * groups)


def solution(mesh):
    in_specs = (P("img", "nrn"), P(None, "nrn", None, None), P(), P())
    out_specs = (P("img", "nrn"), P())
    return jax.shard_map(
        per_device, mesh=mesh, in_specs=in_specs, out_specs=out_specs, check_vma=False
    )
```

```python
import functools

import jax
import jax.numpy as jnp
from jax import lax
from jax.experimental import pallas as pl
from jax.experimental.pallas import tpu as pltpu
from jax.sharding import PartitionSpec as P


live_level = 0.25
ahead_limit = 20 * 2**20
near_limit = 36 * 2**20
far_limit = 32 * 2**20


def xor_pairs(count, mask):
    return [(i, i ^ mask) for i in range(count)]


def outcome(parts, tile, bias):
    result = jnp.dot(jnp.concatenate(parts, axis=1), tile, preferred_element_type=jnp.float32)
    return jnp.maximum(result + bias, 0.0).astype(jnp.bfloat16)


def collapse(value):
    ones = jnp.ones((8, value.shape[1]), jnp.float32)
    return lax.dot_general(
        ones, value, (((1,), (1,)), ((), ())), precision=lax.Precision.HIGHEST, preferred_element_type=jnp.float32
    )


def ahead_kernel(position_ref, own_ref, near_ref, far_ref, weights_ref, inputs, tile, sems):
    position = position_ref[0]
    half, width = inputs.shape[1:]
    rows = own_ref.shape[1] // width
    own_rows = pl.ds(pl.multiple_of(lax.rem(position, 2) * half, half), half)
    for mask, ref in ((0, own_ref.at[own_rows]), (1, near_ref), (2, far_ref)):
        for r in range(rows):
            block = (position ^ mask) * rows + r
            pltpu.make_async_copy(ref.at[:, pl.ds(r * width, width)], inputs.at[block], sems.at[0]).start()
    load = pltpu.make_async_copy(weights_ref.at[0], tile, sems.at[1])
    load.start()
    here = inputs.at[pl.ds(0, 3 * rows)]
    pltpu.make_async_copy(here, here, sems.at[0]).wait()
    load.wait()


def near_kernel(
    position_ref, block_ref, bias_ref, _, tile_ref, cross_ref, near_weights_ref, inputs, first, total_ref, near_tile, sems,
):
    position = position_ref[0]
    _, rows, half, width = first.shape
    deep = near_tile.shape[0] // rows
    for r in range(rows):
        block = (position ^ 3) * rows + r
        pltpu.make_async_copy(cross_ref.at[:, pl.ds(r * width, width)], inputs.at[block], sems.at[0]).start()
    load = pltpu.make_async_copy(near_weights_ref.at[0], near_tile, sems.at[1])
    load.start()
    here = inputs.at[pl.ds(0, rows)]
    pltpu.make_async_copy(here, here, sems.at[0]).wait()

    total = jnp.zeros((half, width), jnp.float32)
    for mask, tile in enumerate((tile_ref, near_tile)):
        if mask:
            load.wait()
        for r in range(rows):
            row = (position ^ mask) * rows + r
            parts = [inputs[block_ref[row * 4 + k]] for k in range(4)]
            first[mask, r] = result = outcome(parts, tile[r * deep : (r + 1) * deep, :], bias_ref[pl.ds(row, 1), :])
            total = total + result.astype(jnp.float32)
    total_ref[...] = total


def far_kernel(
    slots, position_ref, place_ref, block_ref, bias_ref, inputs, near_first, total_ref, weights_ref, near_weights_ref, *refs,
):
    piece_refs, refs = refs[: len(slots)], refs[len(slots) :]
    activations_ref, theirs_ref, sums_ref, first, tiles, second_tiles, outputs, sems = refs
    position = position_ref[0]
    core = lax.rem(position, 2)
    blocks, half, width = first.shape
    rows = near_first.shape[1]
    deep = tiles.shape[1] // rows

    def each_piece(slot, act):
        for i, (ref, own_slot) in enumerate(zip(piece_refs, slots)):
            if own_slot == slot:
                place = place_ref[i]

                @pl.when(place >= 0)
                def _():
                    target = tiles.at[slot - 2, pl.ds(pl.multiple_of(place, 16), ref.shape[0])]
                    act(pltpu.make_async_copy(ref, target, sems.at[6 + i]))

    loads = [
        pltpu.make_async_copy(ref.at[1], second_tiles.at[mask], sems.at[mask])
        for mask, ref in enumerate((weights_ref, near_weights_ref))
    ]
    moves = [
        pltpu.make_async_copy(
            near_first.at[mask], first.at[pl.ds(pl.multiple_of((position ^ mask) * rows, rows), rows)], sems.at[2 + mask]
        )
        for mask in range(2)
    ]
    for slot in (2, 3):
        each_piece(slot, lambda copy: copy.start())
    for copy in loads + moves:
        copy.start()

    def first_layer(step, total):
        for slot in (2, 3):
            @pl.when(step == slot - 2)
            def _():
                each_piece(slot, lambda copy: copy.wait())

        for r in range(rows):
            row = (position ^ (step + 2)) * rows + r
            parts = [inputs[block_ref[row * 4 + k]] for k in range(4)]
            first[row] = result = outcome(parts, tiles[step, r * deep : (r + 1) * deep, :], bias_ref[pl.ds(row, 1), :])
            total = total + result.astype(jnp.float32)
        return total

    sums_ref[0] = collapse(lax.fori_loop(0, 2, first_layer, total_ref[...]))
    for move in moves:
        move.wait()

    def second_layer(step, total):
        mask = 1 - step
        for slot in range(2):
            @pl.when(mask == slot)
            def _():
                loads[slot].wait()

        for r in range(rows):
            row = (position ^ mask) * rows + r + blocks
            parts = [first[block_ref[row * 4 + k]] for k in range(4)]
            result = outcome(parts, second_tiles[mask, r * deep : (r + 1) * deep, :], bias_ref[pl.ds(row, 1), :])
            outputs[mask, :, r * width : (r + 1) * width] = result
            total = total + result.astype(jnp.float32)

        @pl.when(mask == 1)
        def _():
            pltpu.make_async_copy(outputs.at[1], theirs_ref, sems.at[4]).start()

        return total

    second_total = lax.fori_loop(0, 2, second_layer, jnp.zeros((half, width), jnp.float32))
    own_rows = pl.ds(pl.multiple_of(core * half, half), half)
    mine = pltpu.make_async_copy(outputs.at[0], activations_ref.at[own_rows], sems.at[5])
    mine.start()
    sums_ref[1] = collapse(second_total)
    pltpu.make_async_copy(outputs.at[1], theirs_ref, sems.at[4]).wait()
    mine.wait()


def gather_far(weights, position, group, sides, groups):
    rows, width = weights.shape[1:]
    nrn = functools.partial(lax.ppermute, axis_name="nrn")
    both = functools.partial(lax.ppermute, axis_name=("img", "nrn"))
    piece_rows = rows // groups
    splits = 2 if piece_rows % 32 == 0 else 1
    part_rows = piece_rows // splits
    parts = []
    for h in range(splits):
        part = lax.dynamic_slice(weights, (0, group * piece_rows + h * part_rows, 0), (1, part_rows, width))[0]
        weights, part = lax.optimization_barrier((weights, part))
        parts.append(nrn(part, perm=xor_pairs(sides, 2)))
    if groups % 2 or groups > 8:
        piece = jnp.concatenate(parts)
        far = lax.all_gather(piece, "img", axis=0, tiled=True)
        return [far, nrn(far, perm=xor_pairs(sides, 1))], [2, 3], jnp.zeros((2,), jnp.int32), piece

    line = groups // 2
    spot, side = group // 2, group % 2
    upward = lax.rem(position, 2) == 0

    def far_end(z):
        return line - 1 if 2 * z < line else 0

    def pairs(steps, move, direct=False):
        found = []
        for g in range(groups):
            for n in range(sides):
                source = g // 2 - steps if n % 2 == 0 else g // 2 + steps
                target = move(g, n)
                if 0 <= source < line and 0 <= target[0] < groups and not (direct and source == far_end(g // 2)):
                    found.append((g * sides + n, target[0] * sides + target[1]))
        return found

    def onward(g, n):
        return (g + 2 if n % 2 == 0 else g - 2), n

    def beside(g, n):
        return g ^ 1, n

    arrays, slots, places = [], [], []

    last = jnp.where(2 * spot < line, line - 1, 0)

    def keep(array, slot, steps, crossed, passed, offset=0, direct=False):
        step = jnp.where(upward != passed, -steps, steps)
        source = spot + step
        row = (source * 2 + (1 - side if crossed else side)) * piece_rows + offset
        came = (source >= 0) & (source < line)
        if direct:
            came = came & (source != last)
        arrays.append(array)
        slots.append(slot)
        places.append(jnp.where(came, row, -1))

    last_row = (last * 2 + 1 - side) * piece_rows
    extra = lax.dynamic_slice(weights, (0, last_row, 0), (1, piece_rows, width))[0]
    extra = both(extra, perm=[
        (g * sides + n, g * sides + (n ^ 2)) for g in range(groups) for n in range(sides) if (n % 2 == 0) == (g < line)
    ])
    extra_near = nrn(extra, perm=xor_pairs(sides, 1))
    for slot, array, here in ((2, extra, upward), (3, extra_near, ~upward)):
        arrays.append(array)
        slots.append(slot)
        places.append(jnp.where(here == (2 * spot < line), last_row, -1))

    for h, part in enumerate(parts):
        other = both(part, perm=pairs(0, beside))
        keep(other, 2, 0, True, False, h * part_rows)
        keep(nrn(other, perm=xor_pairs(sides, 1)), 3, 0, True, False, h * part_rows)
    piece = jnp.concatenate(parts)
    held = [piece, nrn(piece, perm=xor_pairs(sides, 1))]
    keep(held[0], 2, 0, False, False)
    keep(held[1], 3, 0, False, False)
    for s in range(1, line):
        for h in range(2):
            held[h] = both(held[h], perm=pairs(s - 1, onward))
            keep(held[h], 2 + h, s, False, False)
            keep(nrn(held[h], perm=xor_pairs(sides, 1)), 3 - h, s, False, True)
            moves = pairs(s, beside, direct=h == 1)
            if not moves:
                continue
            other = both(held[h], perm=moves)
            keep(other, 2 + h, s, True, False, direct=h == 1)
            keep(nrn(other, perm=xor_pairs(sides, 1)), 3 - h, s, True, True, direct=h == 1)
    return arrays, slots, jnp.stack(places).astype(jnp.int32), parts[0]


def per_device(images, weights, block_index, bias):
    layers, rows, deep, width = weights.shape
    count, shard = images.shape
    sides = lax.axis_size("nrn")
    groups = lax.axis_size("img")
    assert layers == 2 and sides == 4 and block_index.shape[-1] == 4
    neurons = shard * sides
    position = lax.axis_index("nrn")
    group = lax.axis_index("img")
    core = lax.rem(position, 2)
    half = count // 2
    nrn = functools.partial(lax.ppermute, axis_name="nrn")

    weights = weights.reshape(layers, rows * deep, width)
    pieces, slots, places, arrived = gather_far(weights, position, group, sides, groups)

    tables = position.reshape(1), places, block_index.reshape(-1), bias.reshape(layers * sides * rows, width)
    sent_weights, (place, places, blocks, biases) = lax.optimization_barrier((weights, tables))
    near_weights = nrn(sent_weights, perm=xor_pairs(sides, 1))
    kept = lax.dynamic_slice(images, (core * half, 0), (half, shard))
    far = nrn(kept, perm=xor_pairs(sides, 2))
    late_images, _ = lax.optimization_barrier((images, arrived))
    given = lax.dynamic_slice(late_images, ((1 - core) * half, 0), (half, shard))
    cross = nrn(given, perm=xor_pairs(sides, 3))
    near = nrn(given, perm=xor_pairs(sides, 1))

    any_space = pl.BlockSpec(memory_space=pl.ANY)
    smem = pl.BlockSpec(memory_space=pltpu.SMEM)
    vmem = pl.BlockSpec(memory_space=pltpu.VMEM)
    flops = 2 * half * rows * deep * width
    inputs, tile = pl.pallas_call(
        ahead_kernel,
        out_shape=(
            jax.ShapeDtypeStruct((sides * rows, half, width), jnp.bfloat16),
            jax.ShapeDtypeStruct((rows * deep, width), jnp.bfloat16),
        ),
        in_specs=[smem] + [any_space] * 4,
        out_specs=(vmem,) * 2,
        scratch_shapes=[pltpu.SemaphoreType.DMA((2,))],
        compiler_params=pltpu.CompilerParams(vmem_limit_bytes=ahead_limit),
        cost_estimate=pl.CostEstimate(flops=flops, bytes_accessed=2**23, transcendentals=0),
    )(place, images, near, far, weights)
    inputs, near_first, total = pl.pallas_call(
        near_kernel,
        out_shape=(
            jax.ShapeDtypeStruct((sides * rows, half, width), jnp.bfloat16),
            jax.ShapeDtypeStruct((2, rows, half, width), jnp.bfloat16),
            jax.ShapeDtypeStruct((half, width), jnp.float32),
        ),
        in_specs=[smem] * 2 + [vmem] * 3 + [any_space] * 2,
        out_specs=(vmem,) * 3,
        scratch_shapes=[pltpu.VMEM((rows * deep, width), jnp.bfloat16), pltpu.SemaphoreType.DMA((2,))],
        input_output_aliases={3: 0},
        compiler_params=pltpu.CompilerParams(vmem_limit_bytes=near_limit),
        cost_estimate=pl.CostEstimate(flops=2 * flops, bytes_accessed=2**24, transcendentals=0),
    )(place, blocks, biases, inputs, tile, cross, near_weights)
    activations, theirs, sums = pl.pallas_call(
        functools.partial(far_kernel, slots),
        out_shape=(
            jax.ShapeDtypeStruct((count, shard), jnp.bfloat16),
            jax.ShapeDtypeStruct((half, shard), jnp.bfloat16),
            jax.ShapeDtypeStruct((layers, 8, half), jnp.float32),
        ),
        in_specs=[smem] * 3 + [vmem] * 4 + [any_space] * (2 + len(pieces)),
        out_specs=(any_space, any_space, vmem),
        scratch_shapes=[
            pltpu.VMEM((sides * rows, half, width), jnp.bfloat16),
            pltpu.VMEM((2, rows * deep, width), jnp.bfloat16),
            pltpu.VMEM((2, rows * deep, width), jnp.bfloat16),
            pltpu.VMEM((2, half, shard), jnp.bfloat16),
            pltpu.SemaphoreType.DMA((6 + len(pieces),)),
        ],
        compiler_params=pltpu.CompilerParams(vmem_limit_bytes=far_limit),
        cost_estimate=pl.CostEstimate(flops=4 * flops, bytes_accessed=2**24, transcendentals=0),
    )(place, places, blocks, biases, inputs, near_first, total, weights, near_weights, *pieces)

    back = nrn(theirs, perm=xor_pairs(sides, 1))
    activations = lax.dynamic_update_slice(activations, back, ((1 - core) * half, 0))

    held = [sums]
    for mask in range(1, sides):
        held.append(nrn(sums, perm=xor_pairs(sides, mask)))
    totals = jnp.stack([
        jnp.stack([held[core_mask][0, 0], held[core_mask][1, 0] + held[core_mask ^ 2][1, 0]]) for core_mask in range(2)
    ])
    live = jnp.sum(jnp.minimum(1.0, totals / neurons / live_level), axis=(0, 2))
    if groups & (groups - 1):
        live = lax.psum(live, "img")
    else:
        mask = 1
        while mask < groups:
            live = live + lax.ppermute(live, "img", xor_pairs(groups, mask))
            mask *= 2
    return activations, live / (count * groups)


def solution(mesh):
    in_specs = (P("img", "nrn"), P(None, "nrn", None, None), P(), P())
    out_specs = (P("img", "nrn"), P())
    return jax.shard_map(
        per_device, mesh=mesh, in_specs=in_specs, out_specs=out_specs, check_vma=False
    )
```

```python
import functools

import jax
import jax.numpy as jnp
from jax import lax
from jax.experimental import pallas as pl
from jax.experimental.pallas import tpu as pltpu
from jax.sharding import PartitionSpec as P


live_level = 0.25
ahead_limit = 20 * 2**20
near_limit = 36 * 2**20
far_limit = 32 * 2**20


def xor_pairs(count, mask):
    return [(i, i ^ mask) for i in range(count)]


def outcome(parts, tile, bias):
    result = jnp.dot(jnp.concatenate(parts, axis=1), tile, preferred_element_type=jnp.float32)
    return jnp.maximum(result + bias, 0.0).astype(jnp.bfloat16)


def collapse(value):
    ones = jnp.ones((8, value.shape[1]), jnp.float32)
    return lax.dot_general(
        ones, value, (((1,), (1,)), ((), ())), precision=lax.Precision.HIGHEST, preferred_element_type=jnp.float32
    )


def ahead_kernel(position_ref, own_ref, near_ref, far_ref, weights_ref, inputs, tile, sems):
    position = position_ref[0]
    half, width = inputs.shape[1:]
    rows = own_ref.shape[1] // width
    own_rows = pl.ds(pl.multiple_of(lax.rem(position, 2) * half, half), half)
    for mask, ref in ((0, own_ref.at[own_rows]), (1, near_ref), (2, far_ref)):
        for r in range(rows):
            block = (position ^ mask) * rows + r
            pltpu.make_async_copy(ref.at[:, pl.ds(r * width, width)], inputs.at[block], sems.at[0]).start()
    load = pltpu.make_async_copy(weights_ref.at[0], tile, sems.at[1])
    load.start()
    here = inputs.at[pl.ds(0, 3 * rows)]
    pltpu.make_async_copy(here, here, sems.at[0]).wait()
    load.wait()


def near_kernel(
    position_ref, block_ref, bias_ref, _, tile_ref, cross_ref, near_weights_ref, inputs, first, total_ref, near_tile, sems,
):
    position = position_ref[0]
    _, rows, half, width = first.shape
    deep = near_tile.shape[0] // rows
    for r in range(rows):
        block = (position ^ 3) * rows + r
        pltpu.make_async_copy(cross_ref.at[:, pl.ds(r * width, width)], inputs.at[block], sems.at[0]).start()
    load = pltpu.make_async_copy(near_weights_ref.at[0], near_tile, sems.at[1])
    load.start()
    here = inputs.at[pl.ds(0, rows)]
    pltpu.make_async_copy(here, here, sems.at[0]).wait()

    total = jnp.zeros((half, width), jnp.float32)
    for mask, tile in enumerate((tile_ref, near_tile)):
        if mask:
            load.wait()
        for r in range(rows):
            row = (position ^ mask) * rows + r
            parts = [inputs[block_ref[row * 4 + k]] for k in range(4)]
            first[mask, r] = result = outcome(parts, tile[r * deep : (r + 1) * deep, :], bias_ref[pl.ds(row, 1), :])
            total = total + result.astype(jnp.float32)
    total_ref[...] = total


def far_kernel(
    slots, position_ref, place_ref, block_ref, bias_ref, inputs, near_first, total_ref, weights_ref, near_weights_ref, *refs,
):
    piece_refs, refs = refs[: len(slots)], refs[len(slots) :]
    activations_ref, theirs_ref, sums_ref, first, tiles, second_tiles, outputs, sems = refs
    position = position_ref[0]
    core = lax.rem(position, 2)
    blocks, half, width = first.shape
    rows = near_first.shape[1]
    deep = tiles.shape[1] // rows

    def each_piece(slot, act):
        for i, (ref, own_slot) in enumerate(zip(piece_refs, slots)):
            if own_slot == slot:
                place = place_ref[i]

                @pl.when(place >= 0)
                def _():
                    target = tiles.at[slot - 2, pl.ds(pl.multiple_of(place, 16), ref.shape[0])]
                    act(pltpu.make_async_copy(ref, target, sems.at[6 + i]))

    loads = [
        pltpu.make_async_copy(ref.at[1], second_tiles.at[mask], sems.at[mask])
        for mask, ref in enumerate((weights_ref, near_weights_ref))
    ]
    moves = [
        pltpu.make_async_copy(
            near_first.at[mask], first.at[pl.ds(pl.multiple_of((position ^ mask) * rows, rows), rows)], sems.at[2 + mask]
        )
        for mask in range(2)
    ]
    for slot in (2, 3):
        each_piece(slot, lambda copy: copy.start())
    for copy in loads + moves:
        copy.start()

    total = total_ref[...]
    for step in range(2):
        each_piece(step + 2, lambda copy: copy.wait())
        for r in range(rows):
            row = (position ^ (step + 2)) * rows + r
            parts = [inputs[block_ref[row * 4 + k]] for k in range(4)]
            first[row] = result = outcome(parts, tiles[step, r * deep : (r + 1) * deep, :], bias_ref[pl.ds(row, 1), :])
            total = total + result.astype(jnp.float32)
    sums_ref[0] = collapse(total)
    for move in moves:
        move.wait()

    own_rows = pl.ds(pl.multiple_of(core * half, half), half)
    mine = pltpu.make_async_copy(outputs, activations_ref.at[own_rows], sems.at[4])
    total = jnp.zeros((half, width), jnp.float32)
    for mask, out_ref in enumerate((outputs, theirs_ref)):
        loads[mask].wait()
        for r in range(rows):
            row = (position ^ mask) * rows + r + blocks
            parts = [first[block_ref[row * 4 + k]] for k in range(4)]
            result = outcome(parts, second_tiles[mask, r * deep : (r + 1) * deep, :], bias_ref[pl.ds(row, 1), :])
            out_ref[:, r * width : (r + 1) * width] = result
            total = total + result.astype(jnp.float32)
        if mask == 0:
            mine.start()
    sums_ref[1] = collapse(total)
    mine.wait()


def gather_far(weights, position, group, sides, groups):
    rows, width = weights.shape[1:]
    nrn = functools.partial(lax.ppermute, axis_name="nrn")
    both = functools.partial(lax.ppermute, axis_name=("img", "nrn"))
    piece_rows = rows // groups
    splits = 2 if piece_rows % 32 == 0 else 1
    part_rows = piece_rows // splits
    parts = []
    for h in range(splits):
        part = lax.dynamic_slice(weights, (0, group * piece_rows + h * part_rows, 0), (1, part_rows, width))[0]
        weights, part = lax.optimization_barrier((weights, part))
        parts.append(nrn(part, perm=xor_pairs(sides, 2)))
    if groups % 2 or groups > 8:
        piece = jnp.concatenate(parts)
        far = lax.all_gather(piece, "img", axis=0, tiled=True)
        return [far, nrn(far, perm=xor_pairs(sides, 1))], [2, 3], jnp.zeros((2,), jnp.int32), piece

    line = groups // 2
    spot, side = group // 2, group % 2
    upward = lax.rem(position, 2) == 0

    def far_end(z):
        return line - 1 if 2 * z < line else 0

    def pairs(steps, move, direct=False):
        found = []
        for g in range(groups):
            for n in range(sides):
                source = g // 2 - steps if n % 2 == 0 else g // 2 + steps
                target = move(g, n)
                if 0 <= source < line and 0 <= target[0] < groups and not (direct and source == far_end(g // 2)):
                    found.append((g * sides + n, target[0] * sides + target[1]))
        return found

    def onward(g, n):
        return (g + 2 if n % 2 == 0 else g - 2), n

    def beside(g, n):
        return g ^ 1, n

    arrays, slots, places = [], [], []

    last = jnp.where(2 * spot < line, line - 1, 0)

    def keep(array, slot, steps, crossed, passed, offset=0, direct=False):
        step = jnp.where(upward != passed, -steps, steps)
        source = spot + step
        row = (source * 2 + (1 - side if crossed else side)) * piece_rows + offset
        came = (source >= 0) & (source < line)
        if direct:
            came = came & (source != last)
        arrays.append(array)
        slots.append(slot)
        places.append(jnp.where(came, row, -1))

    last_row = (last * 2 + 1 - side) * piece_rows
    extra = lax.dynamic_slice(weights, (0, last_row, 0), (1, piece_rows, width))[0]
    extra = both(extra, perm=[
        (g * sides + n, g * sides + (n ^ 2)) for g in range(groups) for n in range(sides) if (n % 2 == 0) == (g < line)
    ])
    extra_near = nrn(extra, perm=xor_pairs(sides, 1))
    for slot, array, here in ((2, extra, upward), (3, extra_near, ~upward)):
        arrays.append(array)
        slots.append(slot)
        places.append(jnp.where(here == (2 * spot < line), last_row, -1))

    for h, part in enumerate(parts):
        other = both(part, perm=pairs(0, beside))
        keep(other, 2, 0, True, False, h * part_rows)
        keep(nrn(other, perm=xor_pairs(sides, 1)), 3, 0, True, False, h * part_rows)
    piece = jnp.concatenate(parts)
    held = [piece, nrn(piece, perm=xor_pairs(sides, 1))]
    keep(held[0], 2, 0, False, False)
    keep(held[1], 3, 0, False, False)
    for s in range(1, line):
        for h in range(2):
            held[h] = both(held[h], perm=pairs(s - 1, onward))
            keep(held[h], 2 + h, s, False, False)
            keep(nrn(held[h], perm=xor_pairs(sides, 1)), 3 - h, s, False, True)
            moves = pairs(s, beside, direct=h == 1)
            if not moves:
                continue
            other = both(held[h], perm=moves)
            keep(other, 2 + h, s, True, False, direct=h == 1)
            keep(nrn(other, perm=xor_pairs(sides, 1)), 3 - h, s, True, True, direct=h == 1)
    return arrays, slots, jnp.stack(places).astype(jnp.int32), parts[0]


def per_device(images, weights, block_index, bias):
    layers, rows, deep, width = weights.shape
    count, shard = images.shape
    sides = lax.axis_size("nrn")
    groups = lax.axis_size("img")
    assert layers == 2 and sides == 4 and block_index.shape[-1] == 4
    neurons = shard * sides
    position = lax.axis_index("nrn")
    group = lax.axis_index("img")
    core = lax.rem(position, 2)
    half = count // 2
    nrn = functools.partial(lax.ppermute, axis_name="nrn")

    weights = weights.reshape(layers, rows * deep, width)
    pieces, slots, places, arrived = gather_far(weights, position, group, sides, groups)

    tables = position.reshape(1), places, block_index.reshape(-1), bias.reshape(layers * sides * rows, width)
    sent_weights, (place, places, blocks, biases) = lax.optimization_barrier((weights, tables))
    near_weights = nrn(sent_weights, perm=xor_pairs(sides, 1))
    kept = lax.dynamic_slice(images, (core * half, 0), (half, shard))
    far = nrn(kept, perm=xor_pairs(sides, 2))
    late_images, _ = lax.optimization_barrier((images, arrived))
    given = lax.dynamic_slice(late_images, ((1 - core) * half, 0), (half, shard))
    cross = nrn(given, perm=xor_pairs(sides, 3))
    near = nrn(given, perm=xor_pairs(sides, 1))

    any_space = pl.BlockSpec(memory_space=pl.ANY)
    smem = pl.BlockSpec(memory_space=pltpu.SMEM)
    vmem = pl.BlockSpec(memory_space=pltpu.VMEM)
    flops = 2 * half * rows * deep * width
    inputs, tile = pl.pallas_call(
        ahead_kernel,
        out_shape=(
            jax.ShapeDtypeStruct((sides * rows, half, width), jnp.bfloat16),
            jax.ShapeDtypeStruct((rows * deep, width), jnp.bfloat16),
        ),
        in_specs=[smem] + [any_space] * 4,
        out_specs=(vmem,) * 2,
        scratch_shapes=[pltpu.SemaphoreType.DMA((2,))],
        compiler_params=pltpu.CompilerParams(vmem_limit_bytes=ahead_limit),
        cost_estimate=pl.CostEstimate(flops=flops, bytes_accessed=2**23, transcendentals=0),
    )(place, images, near, far, weights)
    inputs, near_first, total = pl.pallas_call(
        near_kernel,
        out_shape=(
            jax.ShapeDtypeStruct((sides * rows, half, width), jnp.bfloat16),
            jax.ShapeDtypeStruct((2, rows, half, width), jnp.bfloat16),
            jax.ShapeDtypeStruct((half, width), jnp.float32),
        ),
        in_specs=[smem] * 2 + [vmem] * 3 + [any_space] * 2,
        out_specs=(vmem,) * 3,
        scratch_shapes=[pltpu.VMEM((rows * deep, width), jnp.bfloat16), pltpu.SemaphoreType.DMA((2,))],
        input_output_aliases={3: 0},
        compiler_params=pltpu.CompilerParams(vmem_limit_bytes=near_limit),
        cost_estimate=pl.CostEstimate(flops=2 * flops, bytes_accessed=2**24, transcendentals=0),
    )(place, blocks, biases, inputs, tile, cross, near_weights)
    activations, theirs, sums = pl.pallas_call(
        functools.partial(far_kernel, slots),
        out_shape=(
            jax.ShapeDtypeStruct((count, shard), jnp.bfloat16),
            jax.ShapeDtypeStruct((half, shard), jnp.bfloat16),
            jax.ShapeDtypeStruct((layers, 8, half), jnp.float32),
        ),
        in_specs=[smem] * 3 + [vmem] * 4 + [any_space] * (2 + len(pieces)),
        out_specs=(any_space, vmem, vmem),
        scratch_shapes=[
            pltpu.VMEM((sides * rows, half, width), jnp.bfloat16),
            pltpu.VMEM((2, rows * deep, width), jnp.bfloat16),
            pltpu.VMEM((2, rows * deep, width), jnp.bfloat16),
            pltpu.VMEM((half, shard), jnp.bfloat16),
            pltpu.SemaphoreType.DMA((6 + len(pieces),)),
        ],
        compiler_params=pltpu.CompilerParams(vmem_limit_bytes=far_limit),
        cost_estimate=pl.CostEstimate(flops=4 * flops, bytes_accessed=2**24, transcendentals=0),
    )(place, places, blocks, biases, inputs, near_first, total, weights, near_weights, *pieces)

    back = nrn(theirs, perm=xor_pairs(sides, 1))
    activations = lax.dynamic_update_slice(activations, back, ((1 - core) * half, 0))

    held = [sums]
    for mask in range(1, sides):
        held.append(nrn(sums, perm=xor_pairs(sides, mask)))
    totals = jnp.stack([
        jnp.stack([held[core_mask][0, 0], held[core_mask][1, 0] + held[core_mask ^ 2][1, 0]]) for core_mask in range(2)
    ])
    live = jnp.sum(jnp.minimum(1.0, totals / neurons / live_level), axis=(0, 2))
    if groups & (groups - 1):
        live = lax.psum(live, "img")
    else:
        mask = 1
        while mask < groups:
            live = live + lax.ppermute(live, "img", xor_pairs(groups, mask))
            mask *= 2
    return activations, live / (count * groups)


def solution(mesh):
    in_specs = (P("img", "nrn"), P(None, "nrn", None, None), P(), P())
    out_specs = (P("img", "nrn"), P())
    return jax.shard_map(
        per_device, mesh=mesh, in_specs=in_specs, out_specs=out_specs, check_vma=False
    )
```
